32 devices in a mesh: fsdp: 8 (over z, y), tensor: 4 (over x, core).
Axes of the slice: x: 2, y: 2, z: 4, core: 2. Of those that a mesh axis runs over, the one named last changes fastest.
Arguments:
- tokens: bfloat16 [12288, 768], P(('fsdp', 'tensor')), may hold values from -6 to 6
- attn_weight: bfloat16 [3, 768, 768], P(None, 'fsdp', 'tensor'), may hold values from -0.21875 to 0.21875
- query_value_bias: bfloat16 [2, 12, 64], P(None, 'tensor', 'fsdp'), may hold values from -3 to 3
- out_weight: bfloat16 [768, 768], P('tensor', 'fsdp'), may hold values from -1.25 to 1.25
- hidden_weight: bfloat16 [768, 3072], P('fsdp', 'tensor'), may hold values from -0.21875 to 0.21875
- hidden_bias: bfloat16 [48, 64], P('tensor', 'fsdp'), may hold values from -3 to 3
- down_weight: bfloat16 [3072, 768], P('tensor', 'fsdp'), may hold values from -0.109375 to 0.109375
- norm_gains: bfloat16 [2, 768], P(None, 'fsdp'), may hold values from 0.5 to 1.5
- norm_biases: bfloat16 [2, 768], P(None, 'fsdp'), may hold values from -2 to 2
- output_biases: bfloat16 [2, 768], P(None, 'fsdp'), may hold values from -2 to 2
- segment_ids: int32 [12288], P('fsdp'), may hold values from 0 to 15, as said below
- padding: int32 [12288], P('fsdp'), may hold values from 0 to 1, as said below
- cotangent: bfloat16 [12288, 768], P(('fsdp', 'tensor')), may hold values from -6 to 6
Outputs:
- layer_out: bfloat16 [12288, 768], P(('fsdp', 'tensor'))
- tokens_grad: float32 [12288, 768], P(('fsdp', 'tensor'))
- attn_weight_grad: float32 [3, 768, 768], P(None, 'fsdp', 'tensor')
- query_value_bias_grad: float32 [2, 12, 64], P(None, 'tensor', 'fsdp')
- out_weight_grad: float32 [768, 768], P('tensor', 'fsdp')
- hidden_weight_grad: float32 [768, 3072], P('fsdp', 'tensor')
- hidden_bias_grad: float32 [48, 64], P('tensor', 'fsdp')
- down_weight_grad: float32 [3072, 768], P('tensor', 'fsdp')
- norm_gains_grad: float32 [2, 768], P(None, 'fsdp')
- norm_biases_grad: float32 [2, 768], P(None, 'fsdp')
- output_biases_grad: float32 [2, 768], P(None, 'fsdp')
- root_squares: float32 [3], replicated
The draws below stay inside these ranges and needn't reach their ends.
Inputs may be any that keep to these rules, and one draw needn't show every extreme that they name: `segment_ids`: within each sequence of 1536 positions, segment ids start at 0 and rise by one at each new document; every document has 96 to 768 tokens except the last of a sequence, which its end may cut; some document has exactly 768 tokens. Within each sequence, the padding positions (value 0) form a tail of at most 192 positions.
All inputs are finite; a program needn't handle non-finite values.
Results may differ from the reference program's by a relative error of at most 0.013.
The reference program's roundings to bfloat16 on the way count: a program that leaves them out, or rounds other values in their place, can miss the bound.
Values may be sent and summed in bfloat16 or wider, within the bound.
A program may use at most 192 MiB of HBM per device.

```python
import jax
import jax.numpy as jnp
from jax import lax

D = 768
H = 12
DH = 64
FF = 3072
TOK_DEV = 1536
TOKENS = 12288
DOC_MOST = 768
DOC_LEAST = 96


def packed_layout(key):
    seq_count = TOKENS // TOK_DEV
    doc_slots = TOK_DEV // DOC_LEAST + 1
    base_key = jax.random.fold_in(key, 4711)
    key_lengths, key_pick, key_pad = jax.random.split(base_key, 3)
    doc_lengths = jax.random.randint(key_lengths, (seq_count, doc_slots), DOC_LEAST, DOC_MOST + 1, dtype=jnp.int32)
    chosen = jax.random.randint(key_pick, (), 0, seq_count, dtype=jnp.int32)
    seq_numbers = jnp.arange(seq_count, dtype=jnp.int32)
    shortest_seq = (chosen + 1) % seq_count
    doc_lengths = jnp.where((seq_numbers == shortest_seq)[:, None], DOC_LEAST, doc_lengths)
    first_docs = jnp.where(seq_numbers == chosen, DOC_MOST, doc_lengths[:, 0])
    doc_lengths = doc_lengths.at[:, 0].set(first_docs)
    doc_ends = jnp.cumsum(doc_lengths, axis=1)
    positions = jnp.arange(TOK_DEV, dtype=jnp.int32)
    seg_table = jnp.sum((positions[None, :, None] >= doc_ends[:, None, :]).astype(jnp.int32), axis=2)
    pad_lengths = jax.random.randint(key_pad, (seq_count,), 0, TOK_DEV // 8 + 1, dtype=jnp.int32)
    pad_table = (positions[None, :] < TOK_DEV - pad_lengths[:, None]).astype(jnp.int32)
    return (seg_table.reshape(TOKENS).astype(jnp.int32), pad_table.reshape(TOKENS).astype(jnp.int32))


def draw_segment_ids(key, part):
    return packed_layout(key)[0]


def draw_padding(key, part):
    return packed_layout(key)[1]


def levels(stream_key, extent, cuts, low, largest):
    loudness = 1.0
    for position, blocks in cuts:
        heights = jax.random.uniform(jax.random.fold_in(jax.random.fold_in(stream_key, 6), position), (blocks,), jnp.float32, low / len(cuts), largest / len(cuts))
        loudness = loudness * jnp.repeat(jnp.exp(heights), extent[position] // blocks).reshape((-1,) + (1,) * (len(extent) - 1 - position))
    return loudness


def bell_draw(rng, extent, width, limit, cuts=(), kind=jnp.bfloat16):
    level = levels(rng, extent, cuts, -0.22, 0.18) if cuts else 1.0
    values = jax.random.normal(rng, extent, jnp.float32) * width * level
    return jnp.minimum(jnp.maximum(values, -limit), limit).astype(kind)


def setup_inputs(seed: int = 0) -> dict:
    key_list = jax.random.split(jax.random.key(seed), 14)
    tokens = bell_draw(key_list[0], (TOKENS, D), 1.0, 6.0, ((0, 32),))
    attn_weight = bell_draw(key_list[1], (3, D, D), D ** -0.5, 0.21875, ((1, 8), (2, 4)))
    query_value_bias = bell_draw(key_list[2], (2, H, DH), 0.5, 3.0, ((1, 4), (2, 8)))
    out_weight = bell_draw(key_list[3], (D, D), (D // 32) ** -0.5, 1.25, ((0, 4), (1, 8)))
    hidden_weight = bell_draw(key_list[4], (D, FF), D ** -0.5, 0.21875, ((0, 8), (1, 4)))
    hidden_bias = bell_draw(key_list[5], (FF // DH, DH), 0.5, 3.0, ((0, 4), (1, 8)))
    down_weight = bell_draw(key_list[6], (FF, D), FF ** -0.5, 0.109375, ((0, 4), (1, 8)))
    norm_gains = jnp.clip(1.0 + 0.1 * jax.random.normal(key_list[7], (2, D), jnp.float32), 0.5, 1.5).astype(jnp.bfloat16)
    norm_biases = bell_draw(key_list[8], (2, D), 0.3, 2.0, ((1, 8),))
    output_biases = bell_draw(key_list[9], (2, D), 0.3, 2.0, ((1, 8),))
    segment_ids = draw_segment_ids(jax.random.fold_in(key_list[13], 71), 0)
    padding = draw_padding(jax.random.fold_in(key_list[13], 71), 0)
    cotangent = bell_draw(key_list[12], (TOKENS, D), 1.0, 6.0, ((0, 32),))
    return {"tokens": tokens, "attn_weight": attn_weight, "query_value_bias": query_value_bias, "out_weight": out_weight, "hidden_weight": hidden_weight, "hidden_bias": hidden_bias, "down_weight": down_weight, "norm_gains": norm_gains, "norm_biases": norm_biases, "output_biases": output_biases, "segment_ids": segment_ids, "padding": padding, "cotangent": cotangent}


EPSILON = 1e-12
HIGHEST_PRECISION = lax.Precision.HIGHEST

@jax.custom_vjp
def low(v):
    return lax.optimization_barrier(v.astype(jnp.bfloat16)).astype(jnp.float32)

@jax.custom_vjp
def low_back(v):
    return v

def low_keep(v):
    return (low(v), None)

def low_pass(kept, grad):
    return (grad,)

def back_keep(v):
    return (v, None)

def back_low(kept, grad):
    return (low(grad),)
low.defvjp(low_keep, low_pass)
low_back.defvjp(back_keep, back_low)

def layer_norm(hidden, gain_row, shift_row):
    row_mean = lax.optimization_barrier(jnp.mean(hidden, axis=-1, keepdims=True))
    centered = hidden - row_mean
    variance = lax.optimization_barrier(jnp.mean(centered * centered, axis=-1, keepdims=True))
    return centered * lax.rsqrt(variance + EPSILON) * gain_row + shift_row

def matmul_high(left, right):
    return jnp.dot(left, right, precision=HIGHEST_PRECISION)

def attend(queries, all_keys, all_values, seg_ids, pad_flags):
    seq_len = queries.shape[0]
    block_rows = min(512, seq_len)
    positions = jnp.arange(seq_len, dtype=jnp.int32)
    key_live = pad_flags == 1

    def one_block(block_index):
        row_start = block_index * block_rows
        q_rows = lax.dynamic_slice_in_dim(queries, row_start, block_rows, 0)
        seg_rows = lax.dynamic_slice_in_dim(seg_ids, row_start, block_rows, 0)
        pad_rows = lax.dynamic_slice_in_dim(pad_flags, row_start, block_rows, 0)
        pos_rows = row_start + jnp.arange(block_rows, dtype=jnp.int32)
        raw_scores = low_back(jnp.einsum('qhd,khd->hqk', q_rows, all_keys, precision=HIGHEST_PRECISION) * 0.125)
        allowed = (seg_rows[:, None] == seg_ids[None, :]) & key_live[None, :] | (pos_rows[:, None] == positions[None, :])
        masked = jnp.where(allowed[None], raw_scores, -1e+30)
        row_top = lax.optimization_barrier(jnp.max(masked, axis=-1, keepdims=True))
        exp_terms = jnp.exp(masked - row_top)
        attn_probs = exp_terms / lax.optimization_barrier(jnp.sum(exp_terms, axis=-1, keepdims=True))
        context = jnp.einsum('hqk,khd->qhd', low(attn_probs), all_values, precision=HIGHEST_PRECISION)
        return context * pad_rows.astype(context.dtype)[:, None, None]
    blocks = lax.map(jax.checkpoint(one_block), jnp.arange(seq_len // block_rows, dtype=jnp.int32))
    return blocks.reshape(seq_len, -1)

def forward(inputs, attn_w, qv_b, out_w, hidden_w, hidden_b, down_w, gain_rows, shift_rows, bias_rows, seg_ids, pad_flags):
    seq_len = inputs.shape[0]
    projected = jnp.einsum('sd,jde->jse', inputs, attn_w, precision=HIGHEST_PRECISION)
    queries = low(low_back(projected[0] + qv_b[0].reshape(D)))
    all_keys = low(low_back(projected[1]))
    all_values = low(low_back(projected[2] + qv_b[1].reshape(D)))
    context = attend(queries.reshape(seq_len, H, DH), all_keys.reshape(seq_len, H, DH), all_values.reshape(seq_len, H, DH), seg_ids, pad_flags)
    context = low(low_back(context))
    attn_branch = low_back(matmul_high(context, out_w) + bias_rows[0])
    first_norm = layer_norm(inputs + attn_branch, gain_rows[0], shift_rows[0])
    pre_act = low_back(matmul_high(low(first_norm), hidden_w) + hidden_b.reshape(FF))
    acted = jax.nn.gelu(pre_act, approximate=False)
    ff_branch = low_back(matmul_high(low(acted), down_w) + bias_rows[1])
    layer_value = layer_norm(first_norm + ff_branch, gain_rows[1], shift_rows[1])
    return (layer_value, (attn_branch, ff_branch))

def reference(tokens, attn_weight, query_value_bias, out_weight, hidden_weight, hidden_bias, down_weight, norm_gains, norm_biases, output_biases, segment_ids, padding, cotangent):
    weights = tuple((w.astype(jnp.float32) for w in (attn_weight, query_value_bias, out_weight, hidden_weight, hidden_bias, down_weight, norm_gains, norm_biases, output_biases)))
    seq_count = TOKENS // TOK_DEV
    token_seqs = tokens.astype(jnp.float32).reshape(seq_count, TOK_DEV, D)
    cot_seqs = cotangent.astype(jnp.float32).reshape(seq_count, TOK_DEV, D)
    seg_seqs = segment_ids.reshape(seq_count, TOK_DEV)
    pad_seqs = padding.reshape(seq_count, TOK_DEV)

    def per_sequence(carried, item):
        grad_totals, square_totals = carried
        inputs, cot_rows, seg_ids, pad_flags = item

        def local_forward(inputs_in, *weight_list):
            return forward(inputs_in, *weight_list, seg_ids, pad_flags)
        layer_value, pull_back, branches = jax.vjp(local_forward, inputs, *weights, has_aux=True)
        grads = pull_back(cot_rows)
        attn_branch, ff_branch = branches
        live_rows = pad_flags.astype(jnp.float32)[:, None]
        squares = jnp.stack([jnp.sum(live_rows * inputs * inputs), jnp.sum(live_rows * attn_branch * attn_branch), jnp.sum(live_rows * ff_branch * ff_branch)])
        grad_totals = tuple((total + grad for total, grad in zip(grad_totals, grads[1:])))
        return ((grad_totals, square_totals + squares), (layer_value.astype(jnp.bfloat16), grads[0]))
    start_totals = (tuple((jnp.zeros_like(w) for w in weights)), jnp.zeros((3,), jnp.float32))
    (grad_totals, square_totals), (layer_seqs, dtoken_seqs) = lax.scan(per_sequence, start_totals, (token_seqs, cot_seqs, seg_seqs, pad_seqs))
    live_count = jnp.sum(padding.astype(jnp.float32))
    root_values = jnp.sqrt(square_totals / (live_count * D))
    return (layer_seqs.reshape(TOKENS, D), dtoken_seqs.reshape(TOKENS, D), grad_totals[0], grad_totals[1], grad_totals[2], grad_totals[3], grad_totals[4], grad_totals[5], grad_totals[6], grad_totals[7], grad_totals[8], root_values)
```

```python
import functools

import jax
import jax.numpy as jnp
from jax import lax
from jax.experimental import pallas as pl
from jax.experimental.pallas import tpu as pltpu
from jax.sharding import PartitionSpec as P

MESH = pl.DeviceIdType.MESH
DH = 64
EPSILON = 1e-12
MASKED = -1e30
DOC_MOST = 768
BLK = 256
LN_ROWS = 64
wide = jnp.float32
narrow = jnp.bfloat16

PARTS = ("qkv", "out", "up", "down")


def nn(a, b):
    return lax.dot_general(a, b, (((1,), (0,)), ((), ())), preferred_element_type=wide)


def nt(a, b):
    return lax.dot_general(a, b, (((1,), (1,)), ((), ())), preferred_element_type=wide)


def tn(a, b):
    return lax.dot_general(a, b, (((0,), (0,)), ((), ())), preferred_element_type=wide)


def layer_kernel(sizes, *refs):
    fused, n_f, D, F, S, heads, pad_w, shard = sizes
    R = S // 4
    names = list(NAMES_IN) + list(NAMES_OUT) + list(NAMES_SCRATCH)
    r = dict(zip(names, refs))
    tok, cot, slab, vecs, kid_col, seg_row, pad_row = (r[k] for k in NAMES_IN)
    out_ref, dtok_ref, g_out, v_out, vb_out = (r[k] for k in NAMES_OUT)
    X, N, DF, DA = r["X"], r["N"], r["DF"], r["DA"]
    Q, K, V, VT, KT, CTXT, CTX, DC = (r[k] for k in ("Q", "K", "V", "VT", "KT", "CTXT", "CTX", "DC"))
    PR, SC, ACTED, DP, XH, RST, FN = (r[k] for k in ("PR", "SC", "ACTED", "DP", "XH", "RST", "FN"))
    QST, DCST, CT, INNER = r["QST"], r["DCST"], r["CT"], r["INNER"]
    S1, R1, S2, R2 = r["S1"], r["R1"], r["S2"], r["R2"]
    VEC, VA, RVT, VB = r["VEC"], r["VA"], r["RVT"], r["VB"]
    ag_s, ag_r, rs_s, rs_r, vt_s, vt_r = (r[k] for k in ("ag_s", "ag_r", "rs_s", "rs_r", "vt_s", "vt_r"))
    lanes = {"qkv": (0, 3 * pad_w), "out": (3 * pad_w + 2 * F, pad_w), "up": (3 * pad_w, F), "down": (3 * pad_w + F, F)}

    f = lax.axis_index("fsdp")
    t = lax.axis_index("tensor")
    zs = n_f // 2
    z, y = f // 2, f % 2
    t1 = t + 1 - 2 * (t % 2)
    t2 = (t + 2) % 4
    t3 = t1 + 2 - 4 * (t1 // 2)
    yp = z * 2 + 1 - y

    def zpeer(k):
        return ((z + k) % zs) * 2 + y

    def rows(j):
        return pl.ds(pl.multiple_of(j * R, R), R)

    sent = []

    def send(src, dst, ss, rs, to):
        c = pltpu.make_async_remote_copy(
            src_ref=src, dst_ref=dst, send_sem=ss, recv_sem=rs, device_id=to, device_id_type=MESH
        )
        c.start()
        sent.append(c)
        return c

    def arrived(dst, ss, rs):
        pltpu.make_async_remote_copy(
            src_ref=dst, dst_ref=dst, send_sem=ss, recv_sem=rs, device_id=(f, t1), device_id_type=MESH
        ).wait_recv()

    barrier = pltpu.get_barrier_semaphore()
    peers = [(f, t1), (f, t2), (f, t3)]
    if fused:
        peers += [(yp, t)] + [(zpeer(k), t) for k in range(1, zs)]
    for p in peers:
        pl.semaphore_signal(barrier, inc=1, device_id=p, device_id_type=MESH)
    pl.semaphore_wait(barrier, len(peers))

    def gather_start(i, src, full):
        send(src, full.at[rows(t)], ag_s.at[i, 1], ag_r.at[i, 1], (f, t2))
        send(src, full.at[rows(t)], ag_s.at[i, 0], ag_r.at[i, 0], (f, t1))

    def gather_steps(i, full):
        yield t
        arrived(full.at[rows(t1)], ag_s.at[i, 0], ag_r.at[i, 0])
        yield t1
        arrived(full.at[rows(t2)], ag_s.at[i, 1], ag_r.at[i, 1])
        send(full.at[rows(t2)], full.at[rows(t2)], ag_s.at[i, 2], ag_r.at[i, 2], (f, t1))
        yield t2
        arrived(full.at[rows(t3)], ag_s.at[i, 2], ag_r.at[i, 2])
        yield t3

    def scatter_sum(i, part, between=None):
        S1[0] = part(t3).astype(narrow)
        a = send(S1.at[0], R1.at[0], rs_s.at[i, 0], rs_r.at[i, 0], (f, t1))
        far = part(t2)
        arrived(R1.at[0], rs_s.at[i, 0], rs_r.at[i, 0])
        S2[...] = (far + R1[0].astype(wide)).astype(narrow)
        b = send(S2, R2, rs_s.at[i, 2], rs_r.at[i, 2], (f, t2))
        S1[1] = part(t1).astype(narrow)
        c = send(S1.at[1], R1.at[1], rs_s.at[i, 1], rs_r.at[i, 1], (f, t1))
        dtok_ref[...] = part(t)
        if between is not None:
            between()
        arrived(R1.at[1], rs_s.at[i, 1], rs_r.at[i, 1])
        arrived(R2, rs_s.at[i, 2], rs_r.at[i, 2])
        done = (a, b, c)
        for d in done:
            d.wait_send()
        sent[:] = [c for c in sent if all(c is not d for d in done)]

    def summed(at):
        return dtok_ref[at, :] + R1[1, at, :].astype(wide) + R2[at, :].astype(wide)

    gather_start(0, tok, X)
    X[rows(t), :] = tok[...]
    if fused:
        W, VG, w_s, w_r = r["W"], r["VG"], r["w_s"], r["w_r"]

        def shard_rows(ff):
            return pl.ds(pl.multiple_of(ff * shard, shard), shard)

        def w_at(p, ff):
            lo, n = lanes[p]
            return W.at[shard_rows(ff), pl.ds(lo, n)]

        def w_own(p, i):
            lo, n = lanes[p]
            src = slab.at[:, pl.ds(lo, n)]
            for k in range(1, zs):
                send(src, w_at(p, f), w_s.at[i, k - 1], w_r.at[i, k - 1], (zpeer(k), t))
            send(src, w_at(p, f), w_s.at[i, zs - 1], w_r.at[i, zs - 1], (yp, t))

        def w_forward(p, i):
            for k in range(1, zs):
                ff = zpeer(zs - k)
                arrived(w_at(p, ff), w_s.at[i, k - 1], w_r.at[i, k - 1])
                send(w_at(p, ff), w_at(p, ff), w_s.at[i, zs - 1 + k], w_r.at[i, zs - 1 + k], (yp, t))

        def w_finish(p, i):
            arrived(w_at(p, yp), w_s.at[i, zs - 1], w_r.at[i, zs - 1])
            for k in range(1, zs):
                ff = ((z + zs - k) % zs) * 2 + 1 - y
                arrived(w_at(p, ff), w_s.at[i, zs - 1 + k], w_r.at[i, zs - 1 + k])

        n_p = len(PARTS)
        w_own("qkv", 0)
        for k in range(1, zs):
            send(vecs, VG.at[f], w_s.at[n_p, k - 1], w_r.at[n_p, k - 1], (zpeer(k), t))
        send(vecs, VG.at[f], w_s.at[n_p, zs - 1], w_r.at[n_p, zs - 1], (yp, t))
        for i in range(1, n_p):
            w_own(PARTS[i], i)
        W[shard_rows(f), :] = slab[...]
        VG[f] = vecs[...]
        w_forward("qkv", 0)
        for k in range(1, zs):
            ff = zpeer(zs - k)
            arrived(VG.at[ff], w_s.at[n_p, k - 1], w_r.at[n_p, k - 1])
            send(VG.at[ff], VG.at[ff], w_s.at[n_p, zs - 1 + k], w_r.at[n_p, zs - 1 + k], (yp, t))
        w_finish("qkv", 0)
        arrived(VG.at[yp], w_s.at[n_p, zs - 1], w_r.at[n_p, zs - 1])
        for k in range(1, zs):
            ff = ((z + zs - k) % zs) * 2 + 1 - y
            arrived(VG.at[ff], w_s.at[n_p, zs - 1 + k], w_r.at[n_p, zs - 1 + k])
        total = VG[0].astype(wide)
        for k in range(1, n_f):
            total = total + VG[k].astype(wide)
        VEC[...] = total
    else:
        W = slab
        VEC[...] = vecs[...].astype(wide)

    def weight(p):
        lo, n = lanes[p]
        return W[:, lo : lo + n]

    wq = pad_w
    for j in gather_steps(0, X):
        got = nn(X[rows(j), :], weight("qkv"))
        Q[rows(j), :] = (got[:, :wq] + VEC[7:8, :wq]).astype(narrow) * narrow(0.125)
        keys = got[:, wq : 2 * wq]
        values = got[:, 2 * wq : 3 * wq] + VEC[8:9, :wq]
        K[rows(j), :] = keys.astype(narrow)
        V[rows(j), :] = values.astype(narrow)
        KT[:, rows(j)] = keys.T.astype(narrow)
        VT[:, rows(j)] = values.T.astype(narrow)

    nb = S // BLK
    reach = (DOC_MOST + BLK - 2) // BLK
    spans = [(max(0, b - reach), min(nb, b + reach + 1)) for b in range(nb)]
    offs = [sum(hi - lo for lo, hi in spans[:b]) for b in range(nb)]

    def stack_heads(dst, value):
        lane = lax.broadcasted_iota(jnp.int32, value.shape, 1) // DH
        for h in range(heads):
            dst[h * BLK : (h + 1) * BLK, :] = jnp.where(lane == h, value, 0).astype(narrow)

    def krows(kc):
        return pl.ds(pl.multiple_of(kc * BLK, BLK), BLK)

    def attend(b):
        lo, hi = spans[b]
        q0 = b * BLK
        stack_heads(QST, Q[q0 : q0 + BLK, :].astype(wide))
        seg_q = seg_row[:, q0 : q0 + BLK]
        pos_q = q0 + lax.broadcasted_iota(jnp.int32, (1, BLK), 1)

        def scores(kc, top):
            s = nt(K[krows(kc), :], QST[...])
            kid = kid_col[krows(kc), :]
            pos_k = kc * BLK + lax.broadcasted_iota(jnp.int32, (BLK, 1), 0)
            allowed = (kid == seg_q) | (pos_k == pos_q)
            bias = jnp.where(allowed, 0.0, MASKED)
            s = s + jnp.concatenate([bias] * heads, axis=1)
            SC[krows(kc), :] = s
            return jnp.maximum(top, jnp.max(s, axis=0, keepdims=True))

        top = lax.fori_loop(lo, hi, scores, jnp.full((1, heads * BLK), -3e38, wide))

        def exps(kc, total):
            e = jnp.exp(SC[krows(kc), :] - top)
            SC[krows(kc), :] = e
            return total + jnp.sum(e, axis=0, keepdims=True)

        total = lax.fori_loop(lo, hi, exps, jnp.zeros((1, heads * BLK), wide))
        inv = 1.0 / total
        CT[...] = jnp.zeros_like(CT)

        def contexts(kc, carry):
            p = (SC[krows(kc), :] * inv).astype(narrow)
            PR[offs[b] + kc - lo] = p
            for h in range(heads):
                hd = slice(h * DH, (h + 1) * DH)
                CT[hd, :] += nn(VT[hd, krows(kc)], p[:, h * BLK : (h + 1) * BLK])
            return carry

        lax.fori_loop(lo, hi, contexts, 0)
        ct = CT[...] * pad_row[:, q0 : q0 + BLK].astype(wide)
        CTXT[:, q0 : q0 + BLK] = ct
        CTX[q0 : q0 + BLK, :] = ct.T.astype(narrow)

    for b in range(nb):
        attend(b)
        if fused and b == nb // 2:
            w_forward("out", 1)
        if fused and b == nb - 1:
            w_forward("up", 2)
            w_finish("out", 1)

    def mine(at, n=LN_ROWS):
        return kid_col[pl.ds(pl.multiple_of(t * R + at, n), n), :] >= 0

    VA[...] = jnp.zeros_like(VA)
    scatter_sum(0, lambda j: nt(CTX[rows(j), :], weight("out")), (lambda: w_forward("down", 3)) if fused else None)

    def add(row, value):
        VA[row : row + 1, :] += jnp.sum(value, axis=0, keepdims=True)

    def mean(v):
        return jnp.mean(v, axis=-1, keepdims=True)

    def norm(h):
        centered = h - mean(h)
        rstd = lax.rsqrt(mean(centered * centered) + EPSILON)
        return centered * rstd, rstd

    def chunked(body):
        def step(i, carry):
            at = pl.multiple_of(i * LN_ROWS, LN_ROWS)
            body(pl.ds(at, LN_ROWS), pl.ds(pl.multiple_of(t * R + at, LN_ROWS), LN_ROWS), at)
            return carry

        lax.fori_loop(0, R // LN_ROWS, step, 0)

    def first(at, whole_at, start):
        branch = summed(at) + VEC[5:6, :]
        x = tok[at, :].astype(wide)
        xh, rstd = norm(x + branch)
        XH[at, :] = xh
        RST[at, :] = rstd
        fn = xh * VEC[1:2, :] + VEC[3:4, :]
        FN[at, :] = fn
        N[whole_at, :] = fn.astype(narrow)
        live = jnp.where(mine(start), 1.0, 0.0)
        add(7, live * x * x)
        add(8, live * branch * branch)
        add(10, jnp.broadcast_to(live, x.shape))

    chunked(first)
    gather_start(1, N.at[rows(t)], N)
    if fused:
        w_finish("up", 2)

    def up_block(j):
        pre = nn(N[rows(j), :], weight("up")) + VEC[0:1, :F]
        half = 0.5 * (1.0 + lax.erf(pre * 0.7071067811865476))
        ACTED[rows(j), :] = (pre * half).astype(narrow)
        SC[rows(j), :] = half + pre * jnp.exp(-0.5 * pre * pre) * 0.3989422804014327

    for j in gather_steps(1, N):
        up_block(j)
    if fused:
        w_finish("down", 3)
    scatter_sum(1, lambda j: nt(ACTED[rows(j), :], weight("down")))

    def back_norm(dy, xh, rstd, gain):
        d = dy * gain
        return rstd * (d - mean(d) - xh * mean(d * xh))

    def second(at, whole_at, start):
        branch = summed(at) + VEC[6:7, :]
        xh, rstd = norm(FN[at, :] + branch)
        gain = VEC[2:3, :]
        out_ref[at, :] = (xh * gain + VEC[4:5, :]).astype(narrow)
        live = jnp.where(mine(start), 1.0, 0.0)
        add(9, live * branch * branch)
        dy = cot[at, :].astype(wide)
        add(2, dy * xh)
        add(4, dy)
        d_second = back_norm(dy, xh, rstd, gain)
        FN[at, :] = d_second
        low = d_second.astype(narrow)
        DF[whole_at, :] = low
        add(6, low.astype(wide))

    chunked(second)
    gather_start(2, DF.at[rows(t)], DF)

    def d_pre_block(j):
        d = (nn(DF[rows(j), :], weight("down")) * SC[rows(j), :]).astype(narrow)
        DP[rows(j), :] = d
        VA[0:1, :F] += jnp.sum(d.astype(wide), axis=0, keepdims=True)

    for j in gather_steps(2, DF):
        d_pre_block(j)

    G = r["G"] if fused else g_out

    def grad(p, left, right):
        lo, n = lanes[p]
        step_w = 256

        def step(i, carry):
            at = pl.ds(pl.multiple_of(i * step_w, step_w), step_w)
            G[at, lo : lo + n] = tn(left[:, at], right[...]).astype(narrow)
            return carry

        lax.fori_loop(0, D // step_w, step, 0)
        if fused:
            i = PARTS.index(p)
            for zz in range(zs):
                send(
                    G.at[shard_rows(zz * 2 + 1 - y), pl.ds(lo, n)],
                    RY.at[zz, :, pl.ds(lo, n)],
                    g_s.at[i, zz],
                    g_r.at[i, zz],
                    (yp, t),
                )

    def grad_across(p):
        if not fused:
            return
        lo, n = lanes[p]
        i = PARTS.index(p)
        for zz in range(zs):
            arrived(RY.at[zz, :, pl.ds(lo, n)], g_s.at[i, zz], g_r.at[i, zz])
            both = G[shard_rows(zz * 2 + y), lo : lo + n].astype(wide) + RY[zz, :, lo : lo + n].astype(wide)
            RY[zz, :, lo : lo + n] = both.astype(narrow)
        for k in range(1, zs):
            send(
                RY.at[(z + k) % zs, :, pl.ds(lo, n)],
                RZ.at[k - 1, :, pl.ds(lo, n)],
                g_s.at[i, zs + k - 1],
                g_r.at[i, zs + k - 1],
                (zpeer(k), t),
            )

    def grad_finish(p):
        if not fused:
            return
        lo, n = lanes[p]
        i = PARTS.index(p)
        got = RY[z, :, lo : lo + n].astype(wide)
        for k in range(1, zs):
            arrived(RZ.at[k - 1, :, pl.ds(lo, n)], g_s.at[i, zs + k - 1], g_r.at[i, zs + k - 1])
            got = got + RZ[k - 1, :, lo : lo + n].astype(wide)
        g_out[:, lo : lo + n] = got

    if fused:
        RY, RZ, g_s, g_r = (r[k] for k in ("RY", "RZ", "g_s", "g_r"))

    scatter_sum(2, lambda j: nt(DP[rows(j), :], weight("up")), lambda: grad("down", DF, ACTED))

    def first_back(at, whole_at, start):
        dy = FN[at, :] + summed(at)
        xh = XH[at, :]
        add(1, dy * xh)
        add(3, dy)
        d_first = back_norm(dy, xh, RST[at, :], VEC[1:2, :])
        FN[at, :] = d_first
        low = d_first.astype(narrow)
        DA[whole_at, :] = low
        add(5, low.astype(wide))

    chunked(first_back)
    gather_start(3, DA.at[rows(t)], DA)
    for k, tt in enumerate((t1, t2, t3)):
        send(VA, RVT.at[t], vt_s.at[k], vt_r.at[k], (f, tt))
    grad("up", N, DP)

    def d_context_block(j):
        live = jnp.where(kid_col[rows(j), :] >= 0, 1.0, 0.0)
        DC[rows(j), :] = (nn(DA[rows(j), :], weight("out")) * live).astype(narrow)

    for j in gather_steps(3, DA):
        d_context_block(j)
    grad_across("down")

    RVT[t] = VA[...]
    for k, tt in enumerate((t1, t2, t3)):
        arrived(RVT.at[tt], vt_s.at[k], vt_r.at[k])
    both = RVT[0] + RVT[1] + RVT[2] + RVT[3]
    row = lax.broadcasted_iota(jnp.int32, both.shape, 0)
    both = jnp.where(row == 0, VA[...], both)
    if fused:
        RVY, RVZ, vf_s, vf_r = (r[k] for k in ("RVY", "RVZ", "vf_s", "vf_r"))
        RVY[y] = both
        send(RVY.at[y], RVY.at[y], vf_s.at[0], vf_r.at[0], (yp, t))
    else:
        v_out[...] = both

    SC[...] = jnp.zeros_like(SC)
    dk_at, dv_at = slice(0, wq), slice(wq, 2 * wq)

    def attend_back(b):
        lo, hi = spans[b]
        q0 = b * BLK
        stack_heads(QST, Q[q0 : q0 + BLK, :].astype(wide))
        dc = DC[q0 : q0 + BLK, :].astype(wide)
        stack_heads(DCST, dc)
        prod = dc.T * CTXT[:, q0 : q0 + BLK]
        for h in range(heads):
            INNER[:, h * BLK : (h + 1) * BLK] = jnp.sum(prod[h * DH : (h + 1) * DH, :], axis=0, keepdims=True)
        CT[...] = jnp.zeros_like(CT)

        def step(kc, carry):
            p = PR[offs[b] + kc - lo]
            dp = nt(V[krows(kc), :], DCST[...])
            ds = (p.astype(wide) * (dp - INNER[...])).astype(narrow)
            SC[krows(kc), dv_at] += nn(p, DCST[...])
            SC[krows(kc), dk_at] += nn(ds, QST[...])
            for h in range(heads):
                hd = slice(h * DH, (h + 1) * DH)
                CT[hd, :] += nn(KT[hd, krows(kc)], ds[:, h * BLK : (h + 1) * BLK])
            return carry

        lax.fori_loop(lo, hi, step, 0)
        DP[q0 : q0 + BLK, :wq] = (CT[...].T * 0.125).astype(narrow)

    for b in range(nb):
        attend_back(b)
        if b == 0 and fused:
            grad_across("up")
            arrived(RVY.at[1 - y], vf_s.at[0], vf_r.at[0])
            RVZ[z] = RVY[0] + RVY[1]
            for k in range(1, zs):
                send(RVZ.at[z], RVZ.at[z], vf_s.at[k], vf_r.at[k], (zpeer(k), t))
        if b == 1:
            grad("out", DA, CTX)
        if b == 3:
            grad_across("out")
    DP[:, wq : 2 * wq] = SC[:, dk_at].astype(narrow)
    DP[:, 2 * wq : 3 * wq] = SC[:, dv_at].astype(narrow)
    VB[0:1, :] = jnp.sum(DP[:, :wq].astype(wide), axis=0, keepdims=True)
    VB[1:2, :] = jnp.sum(DP[:, 2 * wq : 3 * wq].astype(wide), axis=0, keepdims=True)
    if fused:
        VBG, vb_s, vb_r = r["VBG"], r["vb_s"], r["vb_r"]
        VBG[f] = VB[...]
        ks = list(range(1, n_f))
        for k in ks:
            send(VB, VBG.at[f], vb_s.at[k - 1], vb_r.at[k - 1], ((f + k) % n_f, t))
    else:
        vb_out[...] = VB[...]

    def finish():
        grad("qkv", X, DP.at[:, pl.ds(0, 3 * wq)])
        grad_across("qkv")
        for p in ("down", "up", "out"):
            grad_finish(p)

    scatter_sum(3, lambda j: nt(DP[rows(j), : 3 * wq], weight("qkv")), finish)

    def last(at, whole_at, start):
        dtok_ref[at, :] = FN[at, :] + summed(at)

    chunked(last)
    if fused:
        for k in range(1, zs):
            zz = (z + zs - k) % zs
            arrived(RVZ.at[zz], vf_s.at[k], vf_r.at[k])
        v_out[...] = sum((RVZ[k] for k in range(1, zs)), RVZ[0])
        for k in range(1, n_f):
            arrived(VBG.at[(f + n_f - k) % n_f], vb_s.at[k - 1], vb_r.at[k - 1])
        vb_out[...] = sum((VBG[k] for k in range(1, n_f)), VBG[0])
        grad_finish("qkv")
    for c in sent:
        c.wait_send()


NAMES_IN = ("tok", "cot", "slab", "vecs", "kid_col", "seg_row", "pad_row")
NAMES_OUT = ("out_ref", "dtok_ref", "g_out", "v_out", "vb_out")
NAMES_SCRATCH = []


def scratch_of(fused, n_f, D, F, S, heads, pad_w, shard):
    R = S // 4
    nb = S // BLK
    reach = (DOC_MOST + BLK - 2) // BLK
    tiles = sum(min(nb, b + reach + 1) - max(0, b - reach) for b in range(nb))
    width = 3 * pad_w + 2 * F + pad_w
    zs = n_f // 2
    vm, dma = pltpu.VMEM, pltpu.SemaphoreType.DMA
    out = dict(
        X=vm((S, D), narrow),
        N=vm((S, D), narrow),
        DF=vm((S, D), narrow),
        DA=vm((S, D), narrow),
        Q=vm((S, pad_w), narrow),
        K=vm((S, pad_w), narrow),
        V=vm((S, pad_w), narrow),
        VT=vm((pad_w, S), narrow),
        KT=vm((pad_w, S), narrow),
        CTXT=vm((pad_w, S), wide),
        CTX=vm((S, pad_w), narrow),
        DC=vm((S, pad_w), narrow),
        PR=vm((tiles, BLK, heads * BLK), narrow),
        SC=vm((S, max(heads * BLK, F)), wide),
        ACTED=vm((S, F), narrow),
        DP=vm((S, max(F, 3 * pad_w)), narrow),
        XH=vm((R, D), wide),
        RST=vm((R, 1), wide),
        FN=vm((R, D), wide),
        QST=vm((heads * BLK, pad_w), narrow),
        DCST=vm((heads * BLK, pad_w), narrow),
        CT=vm((pad_w, BLK), wide),
        INNER=vm((1, heads * BLK), wide),
        S1=vm((2, R, D), narrow),
        R1=vm((2, R, D), narrow),
        S2=vm((R, D), narrow),
        R2=vm((R, D), narrow),
        VEC=vm((16, D), wide),
        VA=vm((16, D), wide),
        RVT=vm((4, 16, D), wide),
        VB=vm((8, pad_w), wide),
        ag_s=dma((4, 3)),
        ag_r=dma((4, 3)),
        rs_s=dma((4, 3)),
        rs_r=dma((4, 3)),
        vt_s=dma((3,)),
        vt_r=dma((3,)),
    )
    if fused:
        out.update(
            W=vm((D, width), narrow),
            VG=vm((n_f, 16, D), narrow),
            G=vm((D, width), narrow),
            RY=vm((zs, shard, width), narrow),
            RZ=vm((zs - 1, shard, width), narrow),
            RVY=vm((2, 16, D), wide),
            RVZ=vm((zs, 16, D), wide),
            VBG=vm((n_f, 8, pad_w), wide),
            w_s=dma((5, 2 * zs - 1)),
            w_r=dma((5, 2 * zs - 1)),
            g_s=dma((4, 2 * zs - 1)),
            g_r=dma((4, 2 * zs - 1)),
            vf_s=dma((zs,)),
            vf_r=dma((zs,)),
            vb_s=dma((n_f - 1,)),
            vb_r=dma((n_f - 1,)),
        )
    return out


def shards(
    tokens,
    attn_weight,
    query_value_bias,
    out_weight,
    hidden_weight,
    hidden_bias,
    down_weight,
    norm_gains,
    norm_biases,
    output_biases,
    segment_ids,
    padding,
    cotangent,
):
    n_f = lax.axis_size("fsdp")
    f = lax.axis_index("fsdp")
    R, D = tokens.shape
    S = segment_ids.shape[0]
    F = hidden_weight.shape[1]
    shard = hidden_weight.shape[0]
    heads = query_value_bias.shape[1]
    hw = heads * DH
    pad_w = -(-hw // 128) * 128
    fused = n_f == 8 and shard % 16 == 0
    sizes = (fused, n_f, D, F, S, heads, pad_w, shard)

    def padded(a):
        return jnp.pad(a, ((0, 0), (0, pad_w - hw)))

    slab = jnp.concatenate(
        [padded(attn_weight[0]), padded(attn_weight[1]), padded(attn_weight[2])]
        + [hidden_weight, down_weight.T, padded(out_weight.T)],
        axis=1,
    )
    here = (jnp.arange(n_f) == f).astype(narrow)

    def spread(a):
        return (a[:, None, :] * here[None, :, None]).reshape(a.shape[0], -1)

    def row_of(a):
        flat = a.reshape(1, -1)
        return jnp.pad(flat, ((0, 0), (0, D - flat.shape[1])))

    vecs = jnp.concatenate(
        [row_of(spread(hidden_bias))]
        + [spread(norm_gains), spread(norm_biases), spread(output_biases)]
        + [row_of(spread(query_value_bias[0])), row_of(spread(query_value_bias[1]))]
        + [jnp.zeros((7, D), narrow)],
        axis=0,
    )
    if not fused:
        slab = lax.all_gather(slab, "fsdp", axis=0, tiled=True)
        vecs = lax.psum(vecs.astype(wide), "fsdp").astype(narrow)
    kid_col = jnp.where(padding == 1, segment_ids, -1)[:, None]
    width = slab.shape[1]
    scratch = scratch_of(*sizes)
    NAMES_SCRATCH[:] = list(scratch)
    vm = pl.BlockSpec(memory_space=pltpu.VMEM)
    g_shape = jax.ShapeDtypeStruct((shard, width), wide) if fused else jax.ShapeDtypeStruct((D, width), narrow)
    layer_out, d_tokens, g, v, vb = pl.pallas_call(
        functools.partial(layer_kernel, sizes),
        out_shape=(
            jax.ShapeDtypeStruct((R, D), narrow),
            jax.ShapeDtypeStruct((R, D), wide),
            g_shape,
            jax.ShapeDtypeStruct((16, D), wide),
            jax.ShapeDtypeStruct((8, pad_w), wide),
        ),
        in_specs=[vm] * 7,
        out_specs=[vm] * 5,
        scratch_shapes=list(scratch.values()),
        compiler_params=pltpu.CompilerParams(
            collective_id=0, has_side_effects=True, vmem_limit_bytes=67043328
        ),
    )(tokens, cotangent, slab, vecs, kid_col, segment_ids[None, :], padding[None, :])
    if not fused:
        blocks = g.reshape(n_f, shard, width)
        g = lax.all_to_all(blocks, "fsdp", split_axis=0, concat_axis=0, tiled=True).astype(wide).sum(axis=0)
        v = lax.psum(v, "fsdp")
        vb = lax.psum(vb, "fsdp")

    def mine(a, k):
        return lax.dynamic_slice_in_dim(a.reshape(k, n_f, -1), f, 1, 1)[:, 0]

    d_attn = jnp.stack([g[:, k * pad_w : k * pad_w + hw] for k in range(3)])
    base = 3 * pad_w
    d_bias = mine(vb[:2, :hw].reshape(2 * heads, DH), 2 * heads).reshape(2, heads, -1)
    squares = jnp.sum(v[7:10], axis=1)
    return (
        layer_out,
        d_tokens,
        d_attn,
        d_bias,
        g[:, base + 2 * F : base + 2 * F + hw].T,
        g[:, base : base + F],
        mine(v[0, :F].reshape(-1, DH), F // DH),
        g[:, base + F : base + 2 * F].T,
        mine(v[1:3], 2),
        mine(v[3:5], 2),
        mine(v[5:7], 2),
        jnp.sqrt(squares / (v[10, 0] * D)),
    )


def solution(mesh):
    placed = (
        P(("fsdp", "tensor"), None),
        P(None, "fsdp", "tensor"),
        P(None, "tensor", "fsdp"),
        P("tensor", "fsdp"),
        P("fsdp", "tensor"),
        P("tensor", "fsdp"),
        P("tensor", "fsdp"),
        P(None, "fsdp"),
        P(None, "fsdp"),
        P(None, "fsdp"),
        P("fsdp"),
        P("fsdp"),
        P(("fsdp", "tensor"), None),
    )
    return jax.shard_map(
        shards,
        mesh=mesh,
        in_specs=placed,
        out_specs=(
            P(("fsdp", "tensor"), None),
            P(("fsdp", "tensor"), None),
            P(None, "fsdp", "tensor"),
            P(None, "tensor", "fsdp"),
            P("tensor", "fsdp"),
            P("fsdp", "tensor"),
            P("tensor", "fsdp"),
            P("tensor", "fsdp"),
            P(None, "fsdp"),
            P(None, "fsdp"),
            P(None, "fsdp"),
            P(),
        ),
        check_vma=False,
    )
```
